256 devices in a mesh: items: 4 (over x), users: 64 (over z, y, core).
Axes of the slice: x: 4, y: 4, z: 8, core: 2. Of those that a mesh axis runs over, the one named last changes fastest.
Arguments:
- capsules: bfloat16 [4096, 8, 128], P('users'), may hold values from -6 to 6
- bank: bfloat16 [262144, 128], P(('items', 'users')), may hold values from -0.5 to 0.5
Outputs:
- relative: float32 [4096, 256], P('users', 'items')
- peak: float32 [4096], P('users')
The draws below stay inside these ranges and needn't reach their ends.
All inputs are finite; a program needn't handle non-finite values.
Results may differ from the reference program's by a relative error of at most 0.0003.
Values may be sent and summed in bfloat16 or wider, within the bound.
A program may use at most 64 MiB of HBM per device.

```python
import jax
import jax.numpy as jnp
from jax import lax

E = 128
K = 8
BLOCK = 1024
USERS = 4096
NB = 256
NITEMS = 262144


def block_levels(key, shape, split, least, largest):
    gain, own = 1.0, jax.random.fold_in(key, 6)
    for axis_at, shards_of in split:
        steps = jnp.exp(jax.random.uniform(jax.random.fold_in(own, axis_at), (shards_of,), jnp.float32, least / len(split), largest / len(split)))
        gain = gain * jnp.repeat(steps, shape[axis_at] // shards_of).reshape([-1 if axis == axis_at else 1 for axis in range(len(shape))])
    return gain


def normal_values(key, shape, scale, limit, split=(), kind=jnp.bfloat16):
    array = scale * jax.random.normal(key, shape, jnp.float32)
    if split:
        array = array * block_levels(key, shape, split, -0.22, 0.18)
    return jnp.clip(array, -limit, limit).astype(kind)


def setup_inputs(seed: int = 0) -> dict:
    streams_of = jax.random.split(jax.random.key(seed), 3)
    capsules = normal_values(streams_of[0], (USERS, K, E), 1.0, 6.0, ((0, 64),))
    bank = normal_values(streams_of[1], (NITEMS, E), E ** -0.5, 0.5, ((0, 256),))
    return {"capsules": capsules, "bank": bank}


def reference(capsules, bank):
    flat = capsules.reshape(USERS * K, E)
    blocks = bank.reshape(NB, BLOCK, E)

    def one_block(rows):
        score = jnp.dot(flat, rows.T, preferred_element_type=jnp.float32)
        return jnp.max(score.reshape(USERS, K * BLOCK), axis=1)

    block_peak = lax.map(one_block, blocks).T
    peak = jnp.max(block_peak, axis=1)
    return block_peak - peak[:, None], peak
```

```python
import functools

import jax
import jax.numpy as jnp
from jax import lax
from jax.experimental import pallas as pl
from jax.experimental.pallas import tpu as pltpu
from jax.sharding import PartitionSpec as P

MESH = pl.DeviceIdType.MESH
NX, NY, NZ, NC = 4, 4, 8, 2
K, E, BLOCK = 8, 128, 1024
GROUP = 64
ROWS = GROUP * K
HALF = ROWS // 2
HB = BLOCK // 2

ORDER = (
    "uO00", "wp0", "uP00", "cp1", "uO10", "wp1", "cp2", "wc1", "uP10", "uP11", "uO20",
    "uO21", "wp2", "uP20", "uP21", "uO11", "cp3", "uO30", "wc2", "uO31", "uO32",
    "uP22", "cp4", "wp3", "uP30", "uP31", "uP32", "uO40", "wp4", "uP40", "uP41", "wc3",
    "uP42", "cp5", "uO50", "uO51", "uO52", "uO53", "cp6", "wp5", "uP50", "uP51",
    "uP52", "uP53", "wp6", "uP60", "uP61", "uP62", "uP63", "cp7", "uO70", "uO71",
    "uO72", "uO73", "uO60", "wp7", "uP70", "uP71", "uP72", "uP73", "uO61", "uO62",
    "uO63", "uP43", "uP33", "uO41", "uO42", "uO43", "uO33", "uP23", "uP12", "uP13",
    "uO22", "uO23", "uO12", "uO13", "uP01", "uP02", "uP03", "uO01", "uO02", "uO03",
)

COLUMNS = (((0, 0), (0, 1)), ((1, 0), (2, 1)), ((1, 1), (2, 0)), ((3, 0), (3, 1)))


def kernel(
    caps_ref, bank_ref, rel_ref, peak_ref,
    raw, tmp, own, par, bank, acc, res, recv, xsend, xrecv,
    load_sem, sr, rr, sl, rl, sp, rp, syr, ryr, syl, ryl, so, ro, sx, rx, xsem,
):
    x = lax.axis_index("items")
    u = lax.axis_index("users")
    c = u % 2
    y = (u // 2) % NY
    z = u // (2 * NY)

    def at(zz, yy, cc):
        return (x, (zz * NY + yy) * 2 + cc)

    z_up, z_dn = at((z + 1) % NZ, y, c), at((z + NZ - 1) % NZ, y, c)
    y_up, y_dn = at(z, (y + 1) % NY, c), at(z, (y + NY - 1) % NY, c)
    partner = at(z, y, 1 - c)
    x_peers = [((x + d) % NX, u) for d in (1, 3, 2)]

    def remote(src, dst, send, recv_, to):
        return pltpu.make_async_remote_copy(
            src_ref=src, dst_ref=dst, send_sem=send, recv_sem=recv_,
            device_id=to, device_id_type=MESH,
        )

    load_caps = pltpu.make_async_copy(caps_ref, raw, load_sem.at[0])
    load_bank = pltpu.make_async_copy(bank_ref, bank.at[0], load_sem.at[1])
    load_caps.start()
    load_bank.start()

    barrier = pltpu.get_barrier_semaphore()
    for to in (z_up, z_dn, y_up, y_dn, partner, x_peers[0], x_peers[1]):
        pl.semaphore_signal(barrier, inc=1, device_id=to, device_id_type=MESH)

    load_caps.wait()
    tmp[...] = raw[...].astype(jnp.float32).reshape(ROWS, E)
    for h in range(2):
        for k in range(K):
            rows = tmp[pl.ds(h * HALF + k, HALF // K, stride=K), :]
            own[0, pl.ds(h * HALF + k * (HALF // K), HALF // K), :] = rows.astype(
                jnp.bfloat16
            )
    load_bank.wait()
    pl.semaphore_wait(barrier, 7)

    a, b = pl.ds(0, HALF), pl.ds(HALF, HALF)
    up = {}
    down = {}

    def send_z(k, src_up, src_down):
        up[k] = remote(src_up, own.at[k, a], sr.at[k], rr.at[k], z_up)
        down[k] = remote(src_down, own.at[k, b], sl.at[k], rl.at[k], z_dn)
        up[k].start()
        down[k].start()

    over = {}

    def send_partner(k):
        over[k] = remote(own.at[k], par.at[k], sp.at[k], rp.at[k], partner)
        over[k].start()

    h0, h1 = pl.ds(0, HB), pl.ds(HB, HB)
    right = {}
    left = {}

    def send_y(i, src_up, dst_up, src_down, dst_down):
        right[i] = remote(src_up, dst_up, syr.at[i], ryr.at[i], y_up)
        left[i] = remote(src_down, dst_down, syl.at[i], ryl.at[i], y_dn)
        right[i].start()
        left[i].start()

    send_z(1, own.at[0, a], own.at[0, b])
    send_y(0, bank.at[0, h0], bank.at[1, h0], bank.at[0, h1], bank.at[2, h1])
    send_partner(0)
    send_z(2, own.at[0, b], own.at[0, a])
    send_y(1, bank.at[0, h1], bank.at[1, h1], bank.at[0, h0], bank.at[2, h0])
    for to in x_peers[:2]:
        pl.semaphore_signal(xsem, inc=1, device_id=to, device_id_type=MESH)

    seen = set()

    def unit(which, k, col):
        capsules = (own if which == 0 else par)[k]
        for j, h in COLUMNS[col]:
            items = bank[j, pl.ds(h * HB, HB), :]
            score = lax.dot_general(
                items, capsules, (((1,), (1,)), ((), ())),
                preferred_element_type=jnp.float32,
            )
            top = jnp.max(score.reshape(HB // 8, 8, ROWS), axis=0)
            for half in range(2):
                lo = half * HALF
                v = jnp.maximum(top[:, lo : lo + 128], top[:, lo + 128 : lo + 256])
                if (which, k, j) in seen:
                    v = jnp.maximum(v, acc[which, k, half, j])
                acc[which, k, half, j] = v
            seen.add((which, k, j))

    lane = lax.broadcasted_iota(jnp.int32, (8, 128), 1)
    row = lax.broadcasted_iota(jnp.int32, (8, 128), 0)
    block_row = [((y + d) % NY) * 2 + c for d in (0, 3, 1, 2)]

    def group_tile(which, first, second):
        halves = []
        for k, half in (first, second):
            v = jnp.full((8, 128), -jnp.inf, jnp.float32)
            for j in range(4):
                m = jnp.max(acc[which, k, half, j], axis=0, keepdims=True)
                v = jnp.where(row == block_row[j], m, v)
            v = jnp.maximum(v, pltpu.roll(v, 64, axis=1))
            halves.append(jnp.maximum(v, pltpu.roll(v, 32, axis=1)))
        return jnp.where(lane < 32, halves[0], halves[1])

    back = []

    def give_back(which, d, first, second):
        cc = c if which == 0 else 1 - c
        zz = (z + d) % NZ
        tile = group_tile(which, first, second)
        if which == 0 and d == 0:
            recv[z, c] = tile
            return
        i = len(back)
        res[i] = tile
        copy = remote(res.at[i], recv.at[z, c], so.at[i], ro.at[z, c], at(zz, y, cc))
        copy.start()
        back.append(copy)

    left_to_do = {}
    for op in ORDER:
        if op[0] == "u":
            key = (op[1], (int(op[2]) + 1) // 2)
            left_to_do[key] = left_to_do.get(key, 0) + 1

    for op in ORDER:
        if op[:2] == "cp":
            k = int(op[2])
            up[k].wait_recv()
            down[k].wait_recv()
            if k <= 5:
                send_z(k + 2, own.at[k, a], own.at[k, b])
            send_partner(k)
        elif op[:2] == "wp":
            over[int(op[2])].wait_recv()
        elif op[:2] == "wc":
            i = int(op[2]) - 1
            right[i].wait_recv()
            left[i].wait_recv()
            if i == 0:
                send_y(2, bank.at[1, h0], bank.at[3, h0], bank.at[2, h1], bank.at[3, h1])
        else:
            which, k, col = "OP".index(op[1]), int(op[2]), int(op[3])
            unit(which, k, col)
            d = (k + 1) // 2
            left_to_do[(op[1], d)] -= 1
            if left_to_do[(op[1], d)] == 0:
                if d == 0:
                    give_back(which, 0, (0, 0), (0, 1))
                elif d == 4:
                    give_back(which, 4, (7, 0), (7, 1))
                else:
                    give_back(which, NZ - d, (2 * d - 1, 0), (2 * d, 0))
                    give_back(which, d, (2 * d, 1), (2 * d - 1, 1))

    for dz in range(NZ):
        for dc in range(NC):
            if dz or dc:
                zz, cc = (z + dz) % NZ, (c + dc) % 2
                remote(
                    res.at[0], recv.at[zz, cc], so.at[0], ro.at[zz, cc], partner
                ).wait_recv()
    table = jnp.maximum(recv[:, 0], recv[:, 1])
    top = jnp.max(jnp.max(table, axis=0), axis=0, keepdims=True)
    xsend[...] = jnp.broadcast_to(top, (8, 128))
    pl.semaphore_wait(xsem, 2)
    over_x = [
        remote(xsend, xrecv.at[i], sx.at[i], rx.at[i], to)
        for i, to in enumerate(x_peers)
    ]
    for copy in over_x:
        copy.start()
    for copy in over_x:
        copy.wait_recv()
    peak = jnp.maximum(
        jnp.maximum(xsend[...], xrecv[0]), jnp.maximum(xrecv[1], xrecv[2])
    )
    relative = (table - peak[None]).reshape(NZ * 8, 128)
    rel_ref[...] = relative.T[:GROUP, :]
    peak_ref[...] = peak[:1, :]

    for copies in (up, down, over, right, left):
        for copy in copies.values():
            copy.wait_send()
    for copy in back + over_x:
        copy.wait_send()


def per_device(capsules, bank):
    vmem = pltpu.VMEM
    dma = pltpu.SemaphoreType.DMA
    relative, peak = pl.pallas_call(
        kernel,
        out_shape=(
            jax.ShapeDtypeStruct((GROUP, NZ * 8), jnp.float32),
            jax.ShapeDtypeStruct((1, 128), jnp.float32),
        ),
        in_specs=[pl.BlockSpec(memory_space=pl.ANY)] * 2,
        out_specs=(
            pl.BlockSpec(memory_space=pltpu.VMEM),
            pl.BlockSpec(memory_space=pltpu.VMEM),
        ),
        scratch_shapes=[
            vmem((GROUP, K, E), jnp.bfloat16),
            vmem((ROWS, E), jnp.float32),
            vmem((8, ROWS, E), jnp.bfloat16),
            vmem((8, ROWS, E), jnp.bfloat16),
            vmem((4, BLOCK, E), jnp.bfloat16),
            vmem((2, 8, 2, 4, 8, 128), jnp.float32),
            vmem((15, 8, 128), jnp.float32),
            vmem((NZ, NC, 8, 128), jnp.float32),
            vmem((8, 128), jnp.float32),
            vmem((3, 8, 128), jnp.float32),
            dma((2,)),
            dma((8,)), dma((8,)), dma((8,)), dma((8,)), dma((8,)), dma((8,)),
            dma((3,)), dma((3,)), dma((3,)), dma((3,)),
            dma((15,)), dma((NZ, NC)),
            dma((3,)), dma((3,)),
            pltpu.SemaphoreType.REGULAR,
        ],
        compiler_params=pltpu.CompilerParams(collective_id=0, has_side_effects=True),
    )(capsules, bank)
    return relative, peak[0, :GROUP]


def solution(mesh):
    return jax.shard_map(
        per_device,
        mesh=mesh,
        in_specs=(P("users", None, None), P(("items", "users"), None)),
        out_specs=(P("users", "items"), P("users")),
        check_vma=False,
    )
```

```python
import jax
import jax.numpy as jnp
from jax import lax
from jax.experimental import pallas as pl
from jax.experimental.pallas import tpu as pltpu
from jax.sharding import PartitionSpec as P

MESH = pl.DeviceIdType.MESH
NX, NY, NZ, NC = 4, 4, 8, 2
K, E, BLOCK = 8, 128, 1024
GROUP = 64
ROWS = GROUP * K
HALF = ROWS // 2
QB = BLOCK // 4

SEGMENTS = (
    ((), ("O0:0",)),
    (("p0",), ("P0:0",)),
    (("o1", "c1",), ("O1:01",)),
    ((), ("P0:1", "O0:1",)),
    (("p1",), ("P1:01",)),
    (("o2", "c2",), ("O2:012", "P1:2", "O1:2",)),
    ((), ("P0:2", "O0:2",)),
    (("c3", "p2",), ("P2:0123", "O2:3", "P1:3", "O1:3",)),
    (("o3", "c4",), ("O3:01234", "P2:4", "O2:4", "P1:4", "O1:4",)),
    (("o4", "c5", "p3",), ("O4:012345", "P3:012",)),
    (("c6", "p4",), ("P4:0123456", "O4:6", "P3:34",)),
    (("o5",), ("O5:0123456", "P3:56", "O3:5",)),
    (("o6", "p5",), ("O6:0123456", "P5:01",)),
    (("p6",), ("P6:0123456", "P5:234",)),
    (("o7",), ("O7:0123456", "P5:56", "O3:6",)),
    (("p7",), ("P7:0123456", "P2:56", "O2:5",)),
    ((), ("O2:6", "P1:56", "O1:56",)),
    ((), ("P0:3456",)),
    ((), ("O0:3456",)),
)

COLUMNS = (
    ((0, 0, BLOCK),),
    ((1, 0, QB), (2, 3 * QB, QB)),
    ((1, QB, QB), (2, 2 * QB, QB)),
    ((1, 2 * QB, QB), (2, QB, QB)),
    ((1, 3 * QB, QB), (2, 0, QB)),
    ((3, 0, QB), (3, 3 * QB, QB)),
    ((3, QB, QB), (3, 2 * QB, QB)),
)


def groups_of(d):
    if d == 0:
        return ((0, (0, 0), (0, 1)),)
    if d == 4:
        return ((4, (7, 0), (7, 1)),)
    lo, hi = 2 * d - 1, 2 * d
    return ((NZ - d, (lo, 0), (hi, 0)), (d, (hi, 1), (lo, 1)))


def kernel(
    caps_ref, bank_ref, rel_ref, peak_ref,
    raw, tmp, own, par, bank, acc, res, recv, xsend, xrecv,
    load_sem, sr, rr, sl, rl, sp, rp, syr, ryr, syl, ryl, so, ro, sx, rx, xsem,
):
    x = lax.axis_index("items")
    u = lax.axis_index("users")
    c = lax.rem(u, NC)
    y = lax.rem(lax.div(u, NC), NY)
    z = lax.div(u, NC * NY)

    def at(zz, yy, cc):
        return (x, (zz * NY + yy) * NC + cc)

    def turn(i, d, n):
        return lax.rem(i + d, n)

    z_up, z_dn = at(turn(z, 1, NZ), y, c), at(turn(z, NZ - 1, NZ), y, c)
    y_up, y_dn = at(z, turn(y, 1, NY), c), at(z, turn(y, NY - 1, NY), c)
    partner = at(z, y, 1 - c)
    x_peers = [(turn(x, d, NX), u) for d in (1, 3, 2)]

    def remote(src, dst, send, recv_, to):
        return pltpu.make_async_remote_copy(
            src_ref=src, dst_ref=dst, send_sem=send, recv_sem=recv_,
            device_id=to, device_id_type=MESH,
        )

    load_caps = pltpu.make_async_copy(caps_ref, raw, load_sem.at[0])
    load_bank = pltpu.make_async_copy(bank_ref, bank.at[0], load_sem.at[1])
    load_caps.start()
    load_bank.start()

    barrier = pltpu.get_barrier_semaphore()
    for to in (z_up, z_dn, y_up, y_dn, partner, x_peers[0], x_peers[1]):
        pl.semaphore_signal(barrier, inc=1, device_id=to, device_id_type=MESH)

    load_caps.wait()
    tmp[...] = raw[...].astype(jnp.float32).reshape(ROWS, E)
    for h in range(2):
        for k in range(K):
            rows = tmp[pl.ds(h * HALF + k, HALF // K, stride=K), :]
            own[0, pl.ds(h * HALF + k * (HALF // K), HALF // K), :] = rows.astype(
                jnp.bfloat16
            )
    load_bank.wait()
    pl.semaphore_wait(barrier, 7)

    a, b = pl.ds(0, HALF), pl.ds(HALF, HALF)
    up, down, over, right, left = {}, {}, {}, {}, {}

    def send_z(k, src_up, src_down):
        up[k] = remote(src_up, own.at[k, a], sr.at[k], rr.at[k], z_up)
        down[k] = remote(src_down, own.at[k, b], sl.at[k], rl.at[k], z_dn)
        up[k].start()
        down[k].start()

    def send_partner(k):
        over[k] = remote(own.at[k], par.at[k], sp.at[k], rp.at[k], partner)
        over[k].start()

    def send_y(col, from_up, from_down):
        to_up, to_down = COLUMNS[col]
        slot_up = bank.at[to_up[0], pl.ds(to_up[1], QB)]
        slot_down = bank.at[to_down[0], pl.ds(to_down[1], QB)]
        src_up = bank.at[from_up, pl.ds(to_up[1], QB)]
        src_down = bank.at[from_down, pl.ds(to_down[1], QB)]
        right[col] = remote(src_up, slot_up, syr.at[col], ryr.at[col], y_up)
        left[col] = remote(src_down, slot_down, syl.at[col], ryl.at[col], y_dn)
        right[col].start()
        left[col].start()

    send_z(1, own.at[0, a], own.at[0, b])
    send_y(1, 0, 0)
    send_partner(0)
    send_z(2, own.at[0, b], own.at[0, a])
    for col in (2, 3, 4):
        send_y(col, 0, 0)
    for to in x_peers[:2]:
        pl.semaphore_signal(xsem, inc=1, device_id=to, device_id_type=MESH)

    seen = set()

    def score_slot(which, k, cols):
        pieces = [p for col in cols for p in COLUMNS[col]]
        items = [bank[j, pl.ds(lo, n), :] for j, lo, n in pieces]
        score = lax.dot_general(
            items[0] if len(items) == 1 else jnp.concatenate(items, axis=0),
            (own if which == 0 else par)[k],
            (((1,), (1,)), ((), ())),
            preferred_element_type=jnp.float32,
        )
        tops, start = {}, 0
        for j, _, n in pieces:
            part = score[start : start + n].reshape(n // 8, 8, ROWS)
            top = jnp.max(part, axis=0)
            tops[j] = jnp.maximum(tops[j], top) if j in tops else top
            start += n
        for j, top in tops.items():
            for half in range(2):
                lo = half * HALF
                v = jnp.maximum(top[:, lo : lo + 128], top[:, lo + 128 : lo + 256])
                if (which, k, j) in seen:
                    v = jnp.maximum(v, acc[which, k, half, j])
                acc[which, k, half, j] = v
            seen.add((which, k, j))

    lane = lax.broadcasted_iota(jnp.int32, (8, 128), 1)
    row = lax.broadcasted_iota(jnp.int32, (8, 128), 0)
    block_row = [turn(y, d, NY) * NC + c for d in (0, 3, 1, 2)]

    def group_tile(which, first, second):
        halves = []
        for k, half in (first, second):
            v = jnp.full((8, 128), -jnp.inf, jnp.float32)
            for j in range(4):
                m = jnp.max(acc[which, k, half, j], axis=0, keepdims=True)
                v = jnp.where(row == block_row[j], m, v)
            v = jnp.maximum(v, pltpu.roll(v, 64, axis=1))
            halves.append(jnp.maximum(v, pltpu.roll(v, 32, axis=1)))
        return jnp.where(lane < 32, halves[0], halves[1])

    back = []
    to_send = []

    def finish(which, d):
        cc = c if which == 0 else 1 - c
        for dz, first, second in groups_of(d):
            tile = group_tile(which, first, second)
            if which == 0 and d == 0:
                recv[z, c] = tile
                continue
            i = len(back)
            res[i] = tile
            to = at(turn(z, dz, NZ), y, cc)
            back.append(remote(res.at[i], recv.at[z, c], so.at[i], ro.at[z, c], to))
            to_send.append(back[-1])

    def event(name):
        i = int(name[1])
        if name[0] == "o":
            up[i].wait_recv()
            down[i].wait_recv()
        elif name[0] == "p":
            over[i].wait_recv()
        else:
            right[i].wait_recv()
            left[i].wait_recv()

    def pass_on(name):
        i = int(name[1])
        if name[0] == "o":
            if i <= 5:
                send_z(i + 2, own.at[i, a], own.at[i, b])
            send_partner(i)
        elif name[0] == "c" and i <= 2:
            send_y(i + 4, 1, 2)

    left_over = {}
    for _, units in SEGMENTS:
        for unit in units:
            key = (unit[0], (int(unit[1]) + 1) // 2)
            left_over[key] = left_over.get(key, 0) + len(unit) - 3
    done = []
    for names, units in SEGMENTS:
        for name in names:
            event(name)
        for name in names:
            pass_on(name)
        for copy in to_send:
            copy.start()
        to_send.clear()
        for key in done:
            finish(*key)
        done.clear()
        for unit in units:
            which, k = "OP".index(unit[0]), int(unit[1])
            score_slot(which, k, [int(i) for i in unit[3:]])
            key = (unit[0], (k + 1) // 2)
            left_over[key] -= len(unit) - 3
            if not left_over[key]:
                done.append((which, key[1]))
    for copy in to_send:
        copy.start()
    to_send.clear()
    for key in done:
        finish(*key)

    for dz in range(NZ):
        for dc in range(NC):
            if dz or dc:
                zz, cc = turn(z, dz, NZ), turn(c, dc, NC)
                remote(
                    res.at[0], recv.at[zz, cc], so.at[0], ro.at[zz, cc], partner
                ).wait_recv()
    table = jnp.maximum(recv[:, 0], recv[:, 1])
    top = jnp.max(jnp.max(table, axis=0), axis=0, keepdims=True)
    xsend[...] = jnp.broadcast_to(top, (8, 128))
    pl.semaphore_wait(xsem, 2)
    over_x = [
        remote(xsend, xrecv.at[i], sx.at[i], rx.at[i], to)
        for i, to in enumerate(x_peers)
    ]
    for copy in over_x:
        copy.start()
    for copies in (up, down, over, right, left):
        for copy in copies.values():
            copy.wait_send()
    for copy in back:
        copy.wait_send()
    for copy in over_x:
        copy.wait_recv()
    peak = jnp.maximum(
        jnp.maximum(xsend[...], xrecv[0]), jnp.maximum(xrecv[1], xrecv[2])
    )
    relative = (table - peak[None]).reshape(NZ * 8, 128)
    rel_ref[...] = relative.T[:GROUP, :]
    peak_ref[...] = peak[:1, :]
    for copy in over_x:
        copy.wait_send()


def flush(rel_ref, peak_ref, rel_out, peak_out, row, sem):
    first = pltpu.make_async_copy(rel_ref, rel_out, sem.at[0])
    first.start()
    row[...] = peak_ref[0, :GROUP]
    second = pltpu.make_async_copy(row, peak_out, sem.at[1])
    second.start()
    first.wait()
    second.wait()


def per_device(capsules, bank):
    vmem = pltpu.VMEM
    dma = pltpu.SemaphoreType.DMA
    whole = pl.BlockSpec(memory_space=pltpu.VMEM)
    anywhere = pl.BlockSpec(memory_space=pl.ANY)
    relative, peak = pl.pallas_call(
        kernel,
        out_shape=(
            vmem((GROUP, NZ * 8), jnp.float32),
            vmem((1, 128), jnp.float32),
        ),
        in_specs=[anywhere] * 2,
        out_specs=(whole, whole),
        scratch_shapes=[
            vmem((GROUP, K, E), jnp.bfloat16),
            vmem((ROWS, E), jnp.float32),
            vmem((8, ROWS, E), jnp.bfloat16),
            vmem((8, ROWS, E), jnp.bfloat16),
            vmem((4, BLOCK, E), jnp.bfloat16),
            vmem((2, 8, 2, 4, 8, 128), jnp.float32),
            vmem((15, 8, 128), jnp.float32),
            vmem((NZ, NC, 8, 128), jnp.float32),
            vmem((8, 128), jnp.float32),
            vmem((3, 8, 128), jnp.float32),
            dma((2,)),
            dma((8,)), dma((8,)), dma((8,)), dma((8,)), dma((8,)), dma((8,)),
            dma((7,)), dma((7,)), dma((7,)), dma((7,)),
            dma((15,)), dma((NZ, NC)),
            dma((3,)), dma((3,)),
            pltpu.SemaphoreType.REGULAR,
        ],
        compiler_params=pltpu.CompilerParams(collective_id=0, has_side_effects=True),
    )(capsules, bank)
    return pl.pallas_call(
        flush,
        out_shape=(
            jax.ShapeDtypeStruct((GROUP, NZ * 8), jnp.float32),
            jax.ShapeDtypeStruct((GROUP,), jnp.float32),
        ),
        in_specs=[whole, whole],
        out_specs=(anywhere, anywhere),
        scratch_shapes=[vmem((GROUP,), jnp.float32), dma((2,))],
    )(
        pltpu.with_memory_space_constraint(relative, pltpu.VMEM),
        pltpu.with_memory_space_constraint(peak, pltpu.VMEM),
    )


def solution(mesh):
    return jax.shard_map(
        per_device,
        mesh=mesh,
        in_specs=(P("users", None, None), P(("items", "users"), None)),
        out_specs=(P("users", "items"), P("users")),
        check_vma=False,
    )
```

```python
import jax
import jax.numpy as jnp
from jax import lax
from jax.experimental import pallas as pl
from jax.experimental.pallas import tpu as pltpu
from jax.sharding import PartitionSpec as P

MESH = pl.DeviceIdType.MESH
NX, NY, NZ, NC = 4, 4, 8, 2
K, E, BLOCK = 8, 128, 1024
GROUP = 64
ROWS = GROUP * K
HALF = ROWS // 2
QB = BLOCK // 4
TILE = 256
DEPTH = 4
LAG = 2

SEGMENTS = (
    ((), ("O0:0",)),
    (("p0",), ("P0:0",)),
    (("o1", "c1",), ("O1:01",)),
    ((), ("P0:1", "O0:1",)),
    (("p1",), ("P1:01",)),
    (("o2", "c2",), ("O2:012", "P1:2", "O1:2",)),
    ((), ("P0:2", "O0:2",)),
    (("c3",), ("O2:3", "P1:3", "O1:3",)),
    (("p2",), ("P2:0123",)),
    (("o3", "c4",), ("O3:01234", "P2:4",)),
    ((), ("O2:4", "P1:4", "O1:4",)),
    (("o4", "c5", "p3",), ("O4:012345",)),
    ((), ("P3:012345",)),
    (("c6", "p4",), ("O3:5", "P4:01234",)),
    (("o5",), ("P4:5", "O5:01234",)),
    (("o6",), ("O5:5", "O6:01234",)),
    (("p5",), ("O6:56", "P5:0123",)),
    (("p6",), ("P5:4", "P6:01234",)),
    ((), ("P6:56", "P5:56", "O5:6", "P4:6", "O4:6",)),
    (("o7",), ("P3:6", "O7:01234",)),
    ((), ("O7:56", "O3:6", "P2:56", "O2:56",)),
    (("p7",), ("P1:5", "P7:01234",)),
    ((), ("P7:56", "P1:6", "O1:56",)),
    ((), ("P0:3456",)),
    ((), ("O0:3456",)),
)

COLUMNS = (
    ((0, 0, BLOCK),),
    ((1, 0, QB), (2, 3 * QB, QB)),
    ((1, QB, QB), (2, 2 * QB, QB)),
    ((1, 2 * QB, QB), (2, QB, QB)),
    ((1, 3 * QB, QB), (2, 0, QB)),
    ((3, 0, QB), (3, 3 * QB, QB)),
    ((3, QB, QB), (3, 2 * QB, QB)),
)


def groups_of(d):
    if d == 0:
        return ((0, (0, 0), (0, 1)),)
    if d == 4:
        return ((4, (7, 0), (7, 1)),)
    lo, hi = 2 * d - 1, 2 * d
    return ((NZ - d, (lo, 0), (hi, 0)), (d, (hi, 1), (lo, 1)))


def kernel(
    caps_ref, bank_ref, rel_ref, peak_ref,
    raw, tmp, own, par, bank, acc, res, recv, xsend, xrecv,
    load_sem, sent, came_z, came_p, came_y, came_back, came_x, xsem,
):
    def body(*sums):
        score_blocks(
            caps_ref, bank_ref, rel_ref, peak_ref,
            raw, tmp, own, par, bank, acc, res, recv, xsend, xrecv,
            load_sem, sent, came_z, came_p, came_y, came_back, came_x, xsem,
            (sums[:DEPTH], sums[DEPTH:]),
        )

    tile = [pltpu.ACC(q)((TILE, 2 * E), jnp.float32) for q in (0, 1)]
    pl.run_scoped(body, *[tile[0]] * DEPTH, *[tile[1]] * DEPTH)


def score_blocks(
    caps_ref, bank_ref, rel_ref, peak_ref,
    raw, tmp, own, par, bank, acc, res, recv, xsend, xrecv,
    load_sem, sent, came_z, came_p, came_y, came_back, came_x, xsem,
    sums,
):
    x = lax.axis_index("items")
    u = lax.axis_index("users")
    c = lax.rem(u, NC)
    y = lax.rem(lax.div(u, NC), NY)
    z = lax.div(u, NC * NY)

    def at(zz, yy, cc):
        return (x, (zz * NY + yy) * NC + cc)

    def turn(i, d, n):
        return lax.rem(i + d, n)

    z_up, z_dn = at(turn(z, 1, NZ), y, c), at(turn(z, NZ - 1, NZ), y, c)
    y_up, y_dn = at(z, turn(y, 1, NY), c), at(z, turn(y, NY - 1, NY), c)
    partner = at(z, y, 1 - c)
    x_peers = [(turn(x, d, NX), u) for d in (1, 3, 2)]

    def remote(src, dst, send, recv_, to):
        return pltpu.make_async_remote_copy(
            src_ref=src, dst_ref=dst, send_sem=send, recv_sem=recv_,
            device_id=to, device_id_type=MESH,
        )

    load_caps = pltpu.make_async_copy(caps_ref, raw, load_sem.at[0])
    load_bank = pltpu.make_async_copy(bank_ref, bank.at[0], load_sem.at[1])
    load_caps.start()
    load_bank.start()

    barrier = pltpu.get_barrier_semaphore()
    for to in (z_up, z_dn, y_up, y_dn, partner, x_peers[0], x_peers[1]):
        pl.semaphore_signal(barrier, inc=1, device_id=to, device_id_type=MESH)

    load_caps.wait()
    tmp[...] = raw[...].astype(jnp.float32).reshape(ROWS, E)
    for h in range(2):
        for k in range(K):
            rows = tmp[pl.ds(h * HALF + k, HALF // K, stride=K), :]
            own[0, pl.ds(h * HALF + k * (HALF // K), HALF // K), :] = rows.astype(
                jnp.bfloat16
            )
    load_bank.wait()
    pl.semaphore_wait(barrier, 7)

    a, b = pl.ds(0, HALF), pl.ds(HALF, HALF)

    def send_z(k, src_up, src_down):
        up = remote(src_up, own.at[k, a], sent.at[0], came_z.at[k], z_up)
        down = remote(src_down, own.at[k, b], sent.at[0], came_z.at[k], z_dn)
        up.start()
        down.start()

    def send_partner(k):
        over = remote(own.at[k], par.at[k], sent.at[1], came_p.at[k], partner)
        over.start()

    def send_y(col, from_up, from_down):
        to_up, to_down = COLUMNS[col]
        slot_up = bank.at[to_up[0], pl.ds(to_up[1], QB)]
        slot_down = bank.at[to_down[0], pl.ds(to_down[1], QB)]
        src_up = bank.at[from_up, pl.ds(to_up[1], QB)]
        src_down = bank.at[from_down, pl.ds(to_down[1], QB)]
        right = remote(src_up, slot_up, sent.at[2], came_y.at[col], y_up)
        left = remote(src_down, slot_down, sent.at[2], came_y.at[col], y_dn)
        right.start()
        left.start()

    send_z(1, own.at[0, a], own.at[0, b])
    send_y(1, 0, 0)
    send_partner(0)
    send_z(2, own.at[0, b], own.at[0, a])
    for col in (2, 3, 4):
        send_y(col, 0, 0)
    for to in x_peers[:2]:
        pl.semaphore_signal(xsem, inc=1, device_id=to, device_id_type=MESH)

    seen = set()

    zeros = jnp.zeros((TILE, E), jnp.bfloat16)
    flying = []
    count = [0, 0]

    def push(which, k):
        for q in range(2):
            rows = (own if which == 0 else par)[k, pl.ds(q * HALF, HALF), :]
            pltpu.matmul_push_rhs(
                jnp.concatenate([rows, rows], axis=1),
                staging_register=count[1] % 2, mxu_index=q, transpose=True,
            )
        count[1] += 1

    def read_oldest():
        i, which, k, j = flying.pop(0)
        for half in range(2):
            score = pltpu.matmul_pop(sums[half][i])
            top = jnp.max(score.reshape(TILE // 8, 8, 2 * E), axis=0)
            v = jnp.maximum(top[:, :E], top[:, E:])
            if (which, k, j) in seen:
                v = jnp.maximum(v, acc[which, k, half, j])
            acc[which, k, half, j] = v
        seen.add((which, k, j))

    def multiply(which, k, j, lo, register):
        i = count[0] % DEPTH
        items = jnp.concatenate([bank[j, pl.ds(lo, TILE), :], zeros], axis=1)
        for q in range(2):
            pltpu.matmul_acc_lhs(sums[q][i], items, load_staged_rhs=register)
        count[0] += 1
        flying.append((i, which, k, j))
        if len(flying) > LAG:
            read_oldest()

    lane = lax.broadcasted_iota(jnp.int32, (8, 128), 1)
    row = lax.broadcasted_iota(jnp.int32, (8, 128), 0)
    block_row = [turn(y, d, NY) * NC + c for d in (0, 3, 1, 2)]

    def group_tile(which, first, second):
        halves = []
        for k, half in (first, second):
            v = jnp.full((8, 128), -jnp.inf, jnp.float32)
            for j in range(4):
                m = jnp.max(acc[which, k, half, j], axis=0, keepdims=True)
                v = jnp.where(row == block_row[j], m, v)
            v = jnp.maximum(v, pltpu.roll(v, 64, axis=1))
            halves.append(jnp.maximum(v, pltpu.roll(v, 32, axis=1)))
        return jnp.where(lane < 32, halves[0], halves[1])

    back = []
    to_send = []

    def finish(which, d):
        cc = c if which == 0 else 1 - c
        for dz, first, second in groups_of(d):
            tile = group_tile(which, first, second)
            if which == 0 and d == 0:
                recv[z, c] = tile
                continue
            i = len(back)
            res[i] = tile
            to = at(turn(z, dz, NZ), y, cc)
            back.append(remote(res.at[i], recv.at[z, c], sent.at[3], came_back, to))
            to_send.append(back[-1])

    def landed(ref, sem):
        remote(ref, ref, sent.at[0], sem, partner).wait_recv()

    def left_here(ref, sem):
        remote(ref, ref, sem, came_back, partner).wait_send()

    def event(name):
        i = int(name[1])
        if name[0] == "o":
            landed(own.at[i], came_z.at[i])
        elif name[0] == "p":
            landed(par.at[i], came_p.at[i])
        else:
            landed(bank.at[0, pl.ds(0, 2 * QB)], came_y.at[i])

    def pass_on(name):
        i = int(name[1])
        if name[0] == "o":
            if i <= 5:
                send_z(i + 2, own.at[i, a], own.at[i, b])
            send_partner(i)
        elif name[0] == "c" and i <= 2:
            send_y(i + 4, 1, 2)

    visits = []
    for n, (_, units) in enumerate(SEGMENTS):
        for unit in units:
            tiles = [
                (j, lo + t)
                for col in unit[3:]
                for j, lo, rows in COLUMNS[int(col)]
                for t in range(0, rows, TILE)
            ]
            visits.append((n, "OP".index(unit[0]), int(unit[1]), tiles))
    left_over = {}
    for _, which, k, tiles in visits:
        key = (which, (k + 1) // 2)
        left_over[key] = left_over.get(key, 0) + len(tiles)
    arrives = {(0, 0): -1}
    for n, (names, _) in enumerate(SEGMENTS):
        for name in names:
            if name[0] != "c":
                arrives["op".index(name[0]), int(name[1])] = n
    done = []
    pushed = 0
    at_visit = 0
    for n, (names, units) in enumerate(SEGMENTS):
        for name in names:
            event(name)
        for name in names:
            pass_on(name)
        for copy in to_send:
            copy.start()
        to_send.clear()
        ready, done = done, []
        while at_visit < len(visits) and visits[at_visit][0] == n:
            _, which, k, tiles = visits[at_visit]
            if pushed == at_visit:
                push(which, k)
                pushed += 1
            register = at_visit % 2
            for t, (j, lo) in enumerate(tiles):
                multiply(which, k, j, lo, None if t else register)
                if not t and at_visit + 1 < len(visits):
                    after = visits[at_visit + 1][1:3]
                    if arrives[after] <= n:
                        push(*after)
                        pushed += 1
                if len(ready) and t == 1:
                    for key in ready:
                        finish(*key)
                    ready = []
            key = (which, (k + 1) // 2)
            left_over[key] -= len(tiles)
            if not left_over[key]:
                done.append(key)
            at_visit += 1
    while flying:
        read_oldest()
    for copy in to_send:
        copy.start()
    to_send.clear()
    for key in done:
        finish(*key)

    landed(res, came_back)
    table = jnp.maximum(recv[:, 0], recv[:, 1])
    top = jnp.max(jnp.max(table, axis=0), axis=0, keepdims=True)
    xsend[...] = jnp.broadcast_to(top, (8, 128))
    pl.semaphore_wait(xsem, 2)
    over_x = [
        remote(xsend, xrecv.at[i], sent.at[4], came_x, to)
        for i, to in enumerate(x_peers)
    ]
    for copy in over_x:
        copy.start()
    left_here(own.at[pl.ds(0, 7)], sent.at[0])
    left_here(own, sent.at[1])
    left_here(bank.at[pl.ds(0, 3)], sent.at[2])
    left_here(res, sent.at[3])
    landed(xrecv, came_x)
    peak = jnp.maximum(
        jnp.maximum(xsend[...], xrecv[0]), jnp.maximum(xrecv[1], xrecv[2])
    )
    relative = (table - peak[None]).reshape(NZ * 8, 128)
    rel_ref[...] = relative.T[:GROUP, :]
    peak_ref[...] = peak[:1, :]
    left_here(xrecv, sent.at[4])


def flush(rel_ref, peak_ref, rel_out, peak_out, row, sem):
    first = pltpu.make_async_copy(rel_ref, rel_out, sem.at[0])
    first.start()
    row[...] = peak_ref[0, :GROUP]
    second = pltpu.make_async_copy(row, peak_out, sem.at[1])
    second.start()
    first.wait()
    second.wait()


def per_device(capsules, bank):
    vmem = pltpu.VMEM
    dma = pltpu.SemaphoreType.DMA
    whole = pl.BlockSpec(memory_space=pltpu.VMEM)
    anywhere = pl.BlockSpec(memory_space=pl.ANY)
    relative, peak = pl.pallas_call(
        kernel,
        out_shape=(
            vmem((GROUP, NZ * 8), jnp.float32),
            vmem((1, 128), jnp.float32),
        ),
        in_specs=[anywhere] * 2,
        out_specs=(whole, whole),
        scratch_shapes=[
            vmem((GROUP, K, E), jnp.bfloat16),
            vmem((ROWS, E), jnp.float32),
            vmem((8, ROWS, E), jnp.bfloat16),
            vmem((8, ROWS, E), jnp.bfloat16),
            vmem((4, BLOCK, E), jnp.bfloat16),
            vmem((2, 8, 2, 4, 8, 128), jnp.float32),
            vmem((15, 8, 128), jnp.float32),
            vmem((NZ, NC, 8, 128), jnp.float32),
            vmem((8, 128), jnp.float32),
            vmem((3, 8, 128), jnp.float32),
            dma((2,)),
            dma((5,)), dma((8,)), dma((8,)), dma((7,)), dma(()), dma(()),
            pltpu.SemaphoreType.REGULAR,
        ],
        compiler_params=pltpu.CompilerParams(collective_id=0, has_side_effects=True),
    )(capsules, bank)
    return pl.pallas_call(
        flush,
        out_shape=(
            jax.ShapeDtypeStruct((GROUP, NZ * 8), jnp.float32),
            jax.ShapeDtypeStruct((GROUP,), jnp.float32),
        ),
        in_specs=[whole, whole],
        out_specs=(anywhere, anywhere),
        scratch_shapes=[vmem((GROUP,), jnp.float32), dma((2,))],
    )(
        pltpu.with_memory_space_constraint(relative, pltpu.VMEM),
        pltpu.with_memory_space_constraint(peak, pltpu.VMEM),
    )


def solution(mesh):
    return jax.shard_map(
        per_device,
        mesh=mesh,
        in_specs=(P("users", None, None), P(("items", "users"), None)),
        out_specs=(P("users", "items"), P("users")),
        check_vma=False,
    )
```
